32 devices in a mesh: grp: 2 (over x), path: 8 (over z, y), amp: 2 (over core).
Axes of the slice: x: 2, y: 2, z: 4, core: 2. Of those that a mesh axis runs over, the one named last changes fastest.
Arguments:
- left_slabs: bfloat16 [256, 2, 16384], P(('grp', 'path'), None, 'amp'), parts along dimension 0, may hold values from -0.59765625 to 0.59765625
- right_slabs: bfloat16 [256, 2, 8192], P(('grp', 'path'), None, 'amp'), parts along dimension 0, may hold values from -0.59765625 to 0.59765625
- term_index: int32 [256], P(('grp', 'path')), parts along dimension 0, may hold values from 0 to 3
- left_terms: float32 [4, 2, 2, 2], replicated, may hold values from -4.2 to 4.2
- right_terms: float32 [4, 2, 2, 2], replicated, may hold values from -4.2 to 4.2
- left_gates: bfloat16 [2, 2, 128, 128], replicated, may hold values from -0.375 to 0.375
- right_gates: bfloat16 [2, 2, 128, 128], replicated, may hold values from -0.375 to 0.375
Outputs:
- amplitudes: bfloat16 [2, 32768, 8192], P(None, ('grp', 'path'), 'amp'), parts along dimension 1
The draws below stay inside these ranges and needn't reach their ends.
There are 2 independent parts, one for each index of `grp`. The reference program is written for one: setup_inputs(seed, part) draws one part's arguments, and reference() takes and returns one part's arrays. A program takes and returns all parts, laid end to end along the dimension named above; an argument that names none is the same for every part. Nothing has to cross between parts.
All inputs are finite; a program needn't handle non-finite values.
Results may differ from the reference program's by a relative error of at most 0.0081.
Values may be sent and summed in bfloat16 or wider, within the bound.
No kernel may reach another device: no remote copies, remote signals or barrier semaphores. Data moves between devices by JAX's collectives and lax.ppermute only.
A program may use at most 128 MiB of HBM per device.

```python
import jax
import jax.numpy as jnp
from jax import lax

GATE = 128
TERMS = 4
LA = 16384
RA = 8192
PATHS = 128


def place_ends(drawn, own_key, smallest, high):
    place = [jax.random.randint(jax.random.fold_in(own_key, axis), (), 0, length) for axis, length in enumerate(drawn.shape)]
    main_axis = drawn.shape.index(max(drawn.shape))
    beside = place[:main_axis] + [(place[main_axis] + 1) % drawn.shape[main_axis]] + place[main_axis + 1:]
    return drawn.at[tuple(place)].set(smallest).at[tuple(beside)].set(high)


def level_of(stream_key, extent, split, least, high):
    gain, own = 1.0, jax.random.fold_in(stream_key, 6)
    for axis_at, blocks in split:
        steps = jnp.exp(jax.random.uniform(jax.random.fold_in(own, axis_at), (blocks,), jnp.float32, least / len(split), high / len(split)))
        gain = gain * jnp.repeat(steps, extent[axis_at] // blocks).reshape([-1 if axis == axis_at else 1 for axis in range(len(extent))])
    return gain


def gaussian(stream_key, dims, width, reach, shards=(), kind=jnp.bfloat16):
    level = level_of(stream_key, dims, shards, -0.22, 0.18) if shards else 1.0
    values = jax.random.normal(stream_key, dims, jnp.float32) * width * level
    return jnp.minimum(jnp.maximum(values, -reach), reach).astype(kind)


def setup_inputs(seed: int = 0, part: int = 0) -> dict:
    key_list = jax.random.split(jax.random.key(seed), 8)
    part_keys = jax.random.split(jax.random.fold_in(key_list[7], part), 8)
    return {
        "left_slabs": gaussian(part_keys[0], (PATHS, 2, LA), 0.1, 0.59765625, ((0, 8), (2, 2))),
        "right_slabs": gaussian(part_keys[1], (PATHS, 2, RA), 0.1, 0.59765625, ((0, 8), (2, 2))),
        "term_index": place_ends(jax.random.randint(part_keys[2], (PATHS,), 0, TERMS), jax.random.fold_in(part_keys[2], 1), 0, TERMS - 1).astype(jnp.int32),
        "left_terms": gaussian(key_list[3], (TERMS, 2, 2, 2), 0.7, 4.2, (), jnp.float32),
        "right_terms": gaussian(key_list[4], (TERMS, 2, 2, 2), 0.7, 4.2, (), jnp.float32),
        "left_gates": gaussian(key_list[5], (2, 2, GATE, GATE), (2 * GATE) ** -0.5, 0.375),
        "right_gates": gaussian(key_list[6], (2, 2, GATE, GATE), (2 * GATE) ** -0.5, 0.375),
    }


def cut_term(slab, term_mix):
    paths_here, _, length = slab.shape
    values = slab.astype(jnp.float32).reshape(paths_here, 2, length // 2, 2)
    real_rows = values[:, 0]
    imag_rows = values[:, 1]
    real_mix = term_mix[:, 0]
    imag_mix = term_mix[:, 1]
    real_part = jnp.einsum('pkj,pmj->pkm', real_rows, real_mix) - jnp.einsum('pkj,pmj->pkm', imag_rows, imag_mix)
    imag_part = jnp.einsum('pkj,pmj->pkm', real_rows, imag_mix) + jnp.einsum('pkj,pmj->pkm', imag_rows, real_mix)
    return jnp.stack([real_part, imag_part], 1).reshape(paths_here, 2, length).astype(jnp.bfloat16)


def apply_low(slab, gate_mat):
    paths_here, _, length = slab.shape
    gate_width = gate_mat.shape[-1]
    real_rows = slab[:, 0].reshape(-1, gate_width)
    imag_rows = slab[:, 1].reshape(-1, gate_width)
    upper = jnp.concatenate([gate_mat[0].T, gate_mat[1].T], 1)
    lower = jnp.concatenate([-gate_mat[1].T, gate_mat[0].T], 1)
    right_matrix = jnp.concatenate([upper, lower], 0)
    product = jnp.dot(jnp.concatenate([real_rows, imag_rows], 1), right_matrix, preferred_element_type=jnp.float32)
    real_part = product[:, :gate_width].reshape(paths_here, length)
    imag_part = product[:, gate_width:].reshape(paths_here, length)
    return jnp.stack([real_part, imag_part], 1).astype(jnp.bfloat16)


def apply_high(grouped, gate_mat):
    gate_width = gate_mat.shape[-1]
    stacked = jnp.concatenate([grouped[:, 0], grouped[:, 1]], 1)
    upper = jnp.concatenate([gate_mat[0], -gate_mat[1]], 1)
    lower = jnp.concatenate([gate_mat[1], gate_mat[0]], 1)
    left_matrix = jnp.concatenate([upper, lower], 0)
    product = jnp.einsum('mk,nkr->nmr', left_matrix.astype(jnp.float32), stacked.astype(jnp.float32))
    return jnp.stack([product[:, :gate_width], product[:, gate_width:]], 1).astype(jnp.bfloat16)


def contract(left_part, right_part):
    left_stack = jnp.concatenate([left_part[:, 0], left_part[:, 1]], 0)
    right_real = jnp.concatenate([right_part[:, 0], -right_part[:, 1]], 0)
    right_imag = jnp.concatenate([right_part[:, 1], right_part[:, 0]], 0)
    contract_dims = (((0,), (0,)), ((), ()))
    real_part = lax.dot_general(left_stack, right_real, contract_dims, preferred_element_type=jnp.float32)
    imag_part = lax.dot_general(left_stack, right_imag, contract_dims, preferred_element_type=jnp.float32)
    return real_part, imag_part


def mixes(term_index, terms):
    chosen = (term_index[:, None] == jnp.arange(terms.shape[0], dtype=jnp.int32)[None, :]).astype(jnp.float32)
    flat = jnp.dot(chosen, terms.reshape(terms.shape[0], 8), precision=lax.Precision.HIGHEST)
    return flat.reshape(-1, 2, 2, 2)


def reference(left_slabs, right_slabs, term_index, left_terms, right_terms, left_gates, right_gates):
    paths_all = left_slabs.shape[0]
    left = cut_term(left_slabs, mixes(term_index, left_terms))
    left = apply_low(left, left_gates[0])
    left = apply_high(left.reshape(paths_all, 2, GATE, LA // GATE), left_gates[1]).reshape(paths_all, 2, LA)
    right = cut_term(right_slabs, mixes(term_index, right_terms))
    right = apply_low(right, right_gates[0])
    right = apply_high(right.reshape(paths_all, 2, GATE, RA // GATE), right_gates[1]).reshape(paths_all, 2, RA)
    real_part, imag_part = contract(left, right)
    return jnp.stack([real_part, imag_part], 0).astype(jnp.bfloat16)
```

```python
import jax
import jax.numpy as jnp
from jax import lax
from jax.experimental import pallas as pl
from jax.experimental.pallas import tpu as pltpu
from jax.sharding import PartitionSpec as P

F32 = jnp.float32
BF16 = jnp.bfloat16


def iota(shape, dim):
    return lax.broadcasted_iota(jnp.int32, shape, dim)


def one_hot(test):
    return jnp.where(test, 1.0, 0.0).astype(BF16)


def dot(a, b):
    return jnp.dot(a, b, preferred_element_type=F32)


def swap_pairs(x, axis):
    size = x.shape[axis]
    even = iota(x.shape, axis) % 2 == 0
    return jnp.where(even, pltpu.roll(x, size - 1, axis), pltpu.roll(x, 1, axis))


def swap_rows(x):
    rows, width = x.shape
    return swap_pairs(x.reshape(rows // 8, 8, width), 1).reshape(rows, width)


def row_sign(shape):
    return jnp.where(iota(shape, 0) % 2 == 0, -1.0, 1.0).astype(F32)


def stacked_gate(gates_ref, select, place):
    gate_width = gates_ref.shape[-1]
    columns = iota((gate_width, 2 * gate_width), 1)
    real_at = one_hot(columns == place)
    imag_at = one_hot(columns == place + 1)
    real = dot(select, gates_ref[1, 0]).astype(BF16)
    imag = dot(select, gates_ref[1, 1]).astype(BF16)
    top = dot(real, real_at) - dot(imag, imag_at)
    bottom = dot(imag, real_at) + dot(real, imag_at)
    return jnp.concatenate([top, bottom], 0).astype(BF16)


def cut_and_low(rows, path, index_ref, terms_ref, gates_ref):
    width = rows.shape[1]
    base = index_ref[path] * 8
    parity = iota((1, width), 1) % 2 == 0

    def pattern(part, first, second):
        return jnp.where(parity, terms_ref[base + 4 * part + first], terms_ref[base + 4 * part + second])

    sign = row_sign(rows.shape)
    value = rows.astype(F32)
    turned = swap_rows(value) * sign
    cut = (
        value * pattern(0, 0, 3)
        + turned * pattern(1, 0, 3)
        + swap_pairs(value, 1) * pattern(0, 1, 2)
        + swap_pairs(turned, 1) * pattern(1, 1, 2)
    ).astype(BF16)
    gate = gates_ref[0].reshape(2 * width, width)
    low = lax.dot_general(cut, gate, (((1,), (1,)), ((), ())), preferred_element_type=F32)
    return (low[:, :width] + swap_rows(low[:, width:]) * sign).astype(BF16)


def left_kernel(count, index_ref, terms_ref, gates_ref, own_ref, other_ref, *rest):
    out_refs, stage = rest[:count], rest[count]
    paths, _, width = own_ref.shape
    mine, core = lax.axis_index("path"), lax.axis_index("amp")
    half = width // 2
    part = half // count
    which = iota((half, width), 0)
    target = ((which // part) ^ mine) * (2 * part) + core * part + which % part
    select = one_hot(iota((half, width), 1) == target)
    source = iota((width, 2 * width), 0)
    place = ((source // half) ^ core) * width + (source % half) * 2
    matrix = stacked_gate(gates_ref, select, place)
    slots = 2 * paths

    for pair in range(0, paths, 2):
        columns = []
        for path in (pair, pair + 1):
            parts = [
                cut_and_low(ref[path], path, index_ref, terms_ref, gates_ref)
                for ref in (own_ref, other_ref)
            ]
            columns.append(jnp.concatenate(parts, 0))
        turned = dot(matrix, jnp.concatenate(columns, 1))
        for at, path in enumerate((pair, pair + 1)):
            for ri in range(2):
                stage[pl.ds(ri * paths + path, half, stride=slots), :] = turned[
                    ri * half : (ri + 1) * half, at * width : (at + 1) * width
                ]
    for k in range(count):
        rows = stage[k * part * slots : (k + 1) * part * slots, :]
        out_refs[k][...] = rows.astype(BF16).reshape(part, slots, width)


def right_kernel(index_ref, terms_ref, gates_ref, own_ref, other_ref, out_ref, stage):
    paths, _, width = own_ref.shape
    core = lax.axis_index("amp")
    half, quarter = width // 2, width // 4
    which = iota((half, width), 0)
    target = 2 * (core * quarter + which % quarter) + which // quarter
    select = one_hot(iota((half, width), 1) == target)
    source = iota((width, 2 * width), 0)
    group = source // 2
    place = (source % 2) * width + ((group // quarter) ^ core) * half + (group % quarter) * 2
    matrix = stacked_gate(gates_ref, select, place)
    slots = 2 * paths
    front = iota((1, width), 1) < half

    for four in range(0, paths, 4):
        columns = []
        for pair in (four, four + 2):
            first, second = [
                jnp.concatenate(
                    [
                        cut_and_low(ref[path], path, index_ref, terms_ref, gates_ref)
                        for ref in (own_ref, other_ref)
                    ],
                    0,
                ).astype(F32)
                for path in (pair, pair + 1)
            ]
            upper = jnp.where(front, first, pltpu.roll(second, half, 1))
            lower = jnp.where(front, pltpu.roll(first, half, 1), second)
            columns.append(jnp.concatenate([upper, lower], 0).astype(BF16))
        turned = dot(matrix, jnp.concatenate(columns, 1))
        for at, pair in enumerate((four, four + 2)):
            for ri in range(2):
                block = turned[ri * half : (ri + 1) * half, at * width : (at + 1) * width]
                upper, lower = block[:quarter], block[quarter:]
                stage[pl.ds(ri * paths + pair, quarter, stride=slots), :] = jnp.where(
                    front, upper, pltpu.roll(lower, half, 1)
                )
                stage[pl.ds(ri * paths + pair + 1, quarter, stride=slots), :] = jnp.where(
                    front, pltpu.roll(upper, half, 1), lower
                )
    out_ref[...] = stage[...].astype(BF16).reshape(out_ref.shape)


def arrange_kernel(count, *refs):
    pieces, out_ref = refs[:count], refs[count]
    part, slots, width = pieces[0].shape
    paths = slots // 2
    for j in range(part):
        plain, crossed = [], []
        for piece in pieces:
            block = piece[j].astype(F32)
            real, imag = block[:paths], block[paths:]
            plain += [real, -imag]
            crossed += [imag, real]
        for at, rows in enumerate((plain, crossed)):
            out_ref[at, j * width : (j + 1) * width, :] = jnp.concatenate(rows, 0).T.astype(BF16)


def contract_kernel(count, own_ref, other_ref, *refs):
    pieces, out_ref = refs[:count], refs[count]
    core = lax.axis_index("amp")
    rows = own_ref.shape[1]
    groups = pieces[0].shape[0]
    block = jnp.concatenate(
        [jnp.concatenate([piece[g] for piece in pieces], 0) for g in range(groups)], 1
    )
    tile = min(256, rows)
    for ref, where in ((own_ref, core), (other_ref, 1 - core)):
        for part in range(2):
            for start in range(0, rows, tile):
                at = pl.multiple_of(where * rows + start, tile)
                out_ref[part, pl.ds(at, tile), :] = dot(
                    ref[part, start : start + tile, :], block
                ).astype(BF16)


SMEM = pl.BlockSpec(memory_space=pltpu.SMEM)
VMEM = pl.BlockSpec(memory_space=pltpu.VMEM)


def as_rows(slab, width):
    paths, _, length = slab.shape
    groups = length // width
    return slab.reshape(paths, 2, groups, width).transpose(0, 2, 1, 3).reshape(paths, 2 * groups, width)


def shards(left_slabs, right_slabs, term_index, left_terms, right_terms, left_gates, right_gates):
    width = left_gates.shape[-1]
    count = lax.axis_size("path")
    paths = left_slabs.shape[0]
    slots = 2 * paths

    def swap(x):
        return lax.ppermute(x, "amp", [(0, 1), (1, 0)])

    def hop(x, k):
        return lax.ppermute(x, "path", [(i, i ^ k) for i in range(count)])

    right_other = swap(right_slabs)
    left_other = swap(left_slabs)

    groups = right_slabs.shape[2] // width
    right = pl.pallas_call(
        right_kernel,
        in_specs=[SMEM, SMEM, VMEM, VMEM, VMEM],
        out_specs=VMEM,
        out_shape=jax.ShapeDtypeStruct((groups, slots, width), BF16),
        scratch_shapes=[pltpu.VMEM((groups * slots, width), F32)],
        cost_estimate=pl.CostEstimate(flops=2 * 10**9, bytes_accessed=10**6, transcendentals=0),
        name="right_prep",
    )(term_index, right_terms.reshape(-1), right_gates, as_rows(right_slabs, width), as_rows(right_other, width))

    pieces = {0: right}
    bit = count // 2
    while bit:
        for k in sorted(pieces):
            pieces[k | bit] = hop(pieces[k], bit)
        bit //= 2

    part = width // 2 // count
    left = pl.pallas_call(
        lambda *refs: left_kernel(count, *refs),
        in_specs=[SMEM, SMEM, VMEM, VMEM, VMEM],
        out_specs=[VMEM] * count,
        out_shape=[jax.ShapeDtypeStruct((part, slots, width), BF16)] * count,
        scratch_shapes=[pltpu.VMEM((width // 2 * slots, width), F32)],
        cost_estimate=pl.CostEstimate(flops=4 * 10**9, bytes_accessed=2 * 10**6, transcendentals=0),
        name="left_prep",
    )(term_index, left_terms.reshape(-1), left_gates, as_rows(left_slabs, width), as_rows(left_other, width))
    blocks = [left[0]] + [hop(left[k], k) for k in range(1, count)]
    rows = part * width
    own = pl.pallas_call(
        lambda *refs: arrange_kernel(count, *refs),
        in_specs=[VMEM] * count,
        out_specs=VMEM,
        out_shape=jax.ShapeDtypeStruct((2, rows, count * slots), BF16),
        cost_estimate=pl.CostEstimate(flops=2 * 10**9, bytes_accessed=10**6, transcendentals=0),
        name="left_arrange",
    )(*blocks)
    other = swap(own)

    step = 2
    out = pl.pallas_call(
        lambda *refs: contract_kernel(count, *refs),
        grid=(groups // step,),
        in_specs=[pl.BlockSpec((2, rows, count * slots), lambda i: (0, 0, 0))] * 2
        + [pl.BlockSpec((step, slots, width), lambda i: (i, 0, 0))] * count,
        out_specs=pl.BlockSpec((2, 2 * rows, step * width), lambda i: (0, 0, i)),
        out_shape=jax.ShapeDtypeStruct((2, 2 * rows, groups * width), BF16),
        cost_estimate=pl.CostEstimate(flops=9 * 10**9, bytes_accessed=36 * 10**6, transcendentals=0),
        name="contract",
    )(own, other, *[pieces[k] for k in range(count)])
    return out


def solution(mesh):
    return jax.shard_map(
        shards,
        mesh=mesh,
        in_specs=(
            P(("grp", "path"), None, "amp"),
            P(("grp", "path"), None, "amp"),
            P(("grp", "path")),
            P(),
            P(),
            P(),
            P(),
        ),
        out_specs=P(None, ("grp", "path"), "amp"),
        check_vma=False,
    )
```

```python
import jax
import jax.numpy as jnp
from jax import lax
from jax.experimental import pallas as pl
from jax.experimental.pallas import tpu as pltpu
from jax.sharding import PartitionSpec as P


F32 = jnp.float32
BF16 = jnp.bfloat16


def iota(shape, dim):
    return lax.broadcasted_iota(jnp.int32, shape, dim)


def one_hot(test):
    return jnp.where(test, 1.0, 0.0).astype(BF16)


def dot(a, b):
    return jnp.dot(a, b, preferred_element_type=F32)


def swap_pairs(x, axis):
    size = x.shape[axis]
    even = iota(x.shape, axis) % 2 == 0
    return jnp.where(even, pltpu.roll(x, size - 1, axis), pltpu.roll(x, 1, axis))


def swap_rows(x):
    rows, width = x.shape
    return swap_pairs(x.reshape(rows // 8, 8, width), 1).reshape(rows, width)


def row_sign(shape):
    return jnp.where(iota(shape, 0) % 2 == 0, -1.0, 1.0).astype(F32)


def stacked_gate(gates_ref, select, place):
    gate_width = gates_ref.shape[-1]
    columns = iota((gate_width, 2 * gate_width), 1)
    real_at = one_hot(columns == place)
    imag_at = one_hot(columns == place + 1)
    real = dot(select, gates_ref[1, 0]).astype(BF16)
    imag = dot(select, gates_ref[1, 1]).astype(BF16)
    top = dot(real, real_at) - dot(imag, imag_at)
    bottom = dot(imag, real_at) + dot(real, imag_at)
    return jnp.concatenate([top, bottom], 0).astype(BF16)


def cut_and_low(rows, path, index_ref, terms_ref, gates_ref):
    width = rows.shape[1]
    term = index_ref[path]
    parity = iota((1, width), 1) % 2 == 0

    def pattern(part, first, second):
        return jnp.where(parity, terms_ref[part, 0, first, term], terms_ref[part, 1, second, term])

    sign = row_sign(rows.shape)
    value = rows.astype(F32)
    turned = swap_rows(value) * sign
    cut = (
        value * pattern(0, 0, 1)
        + turned * pattern(1, 0, 1)
        + swap_pairs(value, 1) * pattern(0, 1, 0)
        + swap_pairs(turned, 1) * pattern(1, 1, 0)
    ).astype(BF16)
    gate = gates_ref[0].reshape(2 * width, width)
    low = lax.dot_general(cut, gate, (((1,), (1,)), ((), ())), preferred_element_type=F32)
    return (low[:, :width] + swap_rows(low[:, width:]) * sign).astype(BF16)


def left_kernel(count, index_ref, terms_ref, gates_ref, own_ref, other_ref, *rest):
    out_refs, stage = rest[:count], rest[count]
    paths, _, width = own_ref.shape
    mine, core = lax.axis_index("path"), lax.axis_index("amp")
    half = width // 2
    part = half // count
    which = iota((half, width), 0)
    target = ((which // part) ^ mine) * (2 * part) + core * part + which % part
    select = one_hot(iota((half, width), 1) == target)
    source = iota((width, 2 * width), 0)
    place = ((source // half) ^ core) * width + (source % half) * 2
    matrix = stacked_gate(gates_ref, select, place)
    slots = 2 * paths

    for pair in range(0, paths, 2):
        columns = []
        for path in (pair, pair + 1):
            parts = [
                cut_and_low(ref[path], path, index_ref, terms_ref, gates_ref)
                for ref in (own_ref, other_ref)
            ]
            columns.append(jnp.concatenate(parts, 0))
        turned = dot(matrix, jnp.concatenate(columns, 1))
        for at, path in enumerate((pair, pair + 1)):
            for ri in range(2):
                stage[pl.ds(ri * paths + path, half, stride=slots), :] = turned[
                    ri * half : (ri + 1) * half, at * width : (at + 1) * width
                ]
    for k in range(count):
        rows = stage[k * part * slots : (k + 1) * part * slots, :]
        out_refs[k][...] = rows.astype(BF16).reshape(part, slots, width)


def right_kernel(index_ref, terms_ref, gates_ref, own_ref, other_ref, out_ref, stage):
    paths, _, width = own_ref.shape
    core = lax.axis_index("amp")
    half, quarter = width // 2, width // 4
    which = iota((half, width), 0)
    target = 2 * (core * quarter + which % quarter) + which // quarter
    select = one_hot(iota((half, width), 1) == target)
    source = iota((width, 2 * width), 0)
    group = source // 2
    place = (source % 2) * width + ((group // quarter) ^ core) * half + (group % quarter) * 2
    matrix = stacked_gate(gates_ref, select, place)
    slots = 2 * paths
    front = iota((1, width), 1) < half

    for four in range(0, paths, 4):
        columns = []
        for pair in (four, four + 2):
            first, second = [
                jnp.concatenate(
                    [
                        cut_and_low(ref[path], path, index_ref, terms_ref, gates_ref)
                        for ref in (own_ref, other_ref)
                    ],
                    0,
                ).astype(F32)
                for path in (pair, pair + 1)
            ]
            upper = jnp.where(front, first, pltpu.roll(second, half, 1))
            lower = jnp.where(front, pltpu.roll(first, half, 1), second)
            columns.append(jnp.concatenate([upper, lower], 0).astype(BF16))
        turned = dot(matrix, jnp.concatenate(columns, 1))
        for at, pair in enumerate((four, four + 2)):
            for ri in range(2):
                block = turned[ri * half : (ri + 1) * half, at * width : (at + 1) * width]
                upper, lower = block[:quarter], block[quarter:]
                stage[pl.ds(ri * paths + pair, quarter, stride=slots), :] = jnp.where(
                    front, upper, pltpu.roll(lower, half, 1)
                )
                stage[pl.ds(ri * paths + pair + 1, quarter, stride=slots), :] = jnp.where(
                    front, pltpu.roll(upper, half, 1), lower
                )
    out_ref[...] = stage[...].astype(BF16).reshape(out_ref.shape)


def arrange_kernel(count, *refs):
    pieces, out_ref = refs[:count], refs[count]
    part, slots, width = pieces[0].shape
    paths = slots // 2
    for j in range(part):
        plain, crossed = [], []
        for piece in pieces:
            block = piece[j].astype(F32)
            real, imag = block[:paths], block[paths:]
            plain += [real, -imag]
            crossed += [imag, real]
        for at, rows in enumerate((plain, crossed)):
            out_ref[at, j * width : (j + 1) * width, :] = jnp.concatenate(rows, 0).T.astype(BF16)


def contract_kernel(count, step, own_ref, other_ref, *refs):
    pieces, out_ref = refs[:count], refs[count]
    left, right, staged, in_sems, out_sems = refs[count + 1 :]
    core = lax.axis_index("amp")
    rows = own_ref.shape[1]
    groups, slots, width = pieces[0].shape
    span = step * width
    copies = [
        pltpu.make_async_copy(
            ref, left.at[:, pl.ds(pl.multiple_of(where * rows, rows), rows), :], in_sems.at[at]
        )
        for at, (ref, where) in enumerate(((own_ref, core), (other_ref, 1 - core)))
    ] + [
        pltpu.make_async_copy(piece, right.at[:, pl.ds(k * slots, slots), :], in_sems.at[2 + k])
        for k, piece in enumerate(pieces)
    ]
    for copy in copies:
        copy.start()
    for copy in copies:
        copy.wait()
    buffers = staged.shape[0]

    def write(i, slot):
        place = pl.ds(pl.multiple_of(i * span, span), span)
        return pltpu.make_async_copy(staged.at[slot], out_ref.at[:, :, place], out_sems.at[slot])

    tile = min(256, 2 * rows)

    @pl.loop(0, groups // step)
    def _(i):
        slot = lax.rem(i, buffers)

        @pl.when(i >= buffers)
        def _():
            write(i - buffers, slot).wait()

        block = jnp.concatenate([right[i * step + g] for g in range(step)], 1)
        for part in range(2):
            for start in range(0, 2 * rows, tile):
                staged[slot, part, start : start + tile, :] = dot(
                    left[part, start : start + tile, :], block
                ).astype(BF16)
        write(i, slot).start()

    for i in range(groups // step - buffers, groups // step):
        write(i, i % buffers).wait()


SMEM = pl.BlockSpec(memory_space=pltpu.SMEM)
VMEM = pl.BlockSpec(memory_space=pltpu.VMEM)
ANY = pl.BlockSpec(memory_space=pl.ANY)


def as_rows(slab, width):
    paths, _, length = slab.shape
    groups = length // width
    return slab.reshape(paths, 2, groups, width).transpose(0, 2, 1, 3).reshape(paths, 2 * groups, width)


def shards(left_slabs, right_slabs, term_index, left_terms, right_terms, left_gates, right_gates):
    width = left_gates.shape[-1]
    count = lax.axis_size("path")
    paths = left_slabs.shape[0]
    slots = 2 * paths

    def swap(x):
        return lax.ppermute(x, "amp", [(0, 1), (1, 0)])

    def hop(x, k):
        return lax.ppermute(x, "path", [(i, i ^ k) for i in range(count)])

    right_other = swap(right_slabs)
    left_other = swap(left_slabs)

    groups = right_slabs.shape[2] // width
    right = pl.pallas_call(
        right_kernel,
        in_specs=[SMEM, SMEM, VMEM, VMEM, VMEM],
        out_specs=VMEM,
        out_shape=jax.ShapeDtypeStruct((groups, slots, width), BF16),
        scratch_shapes=[pltpu.VMEM((groups * slots, width), F32)],
        cost_estimate=pl.CostEstimate(flops=2 * 10**9, bytes_accessed=10**6, transcendentals=0),
        compiler_params=pltpu.CompilerParams(vmem_limit_bytes=24 * 2**20),
        name="right_prep",
    )(
        term_index,
        right_terms.transpose(1, 2, 3, 0),
        right_gates,
        as_rows(right_slabs, width),
        as_rows(right_other, width),
    )

    part = width // 2 // count
    left = pl.pallas_call(
        lambda *refs: left_kernel(count, *refs),
        in_specs=[SMEM, SMEM, VMEM, VMEM, VMEM],
        out_specs=[VMEM] * count,
        out_shape=[jax.ShapeDtypeStruct((part, slots, width), BF16)] * count,
        scratch_shapes=[pltpu.VMEM((width // 2 * slots, width), F32)],
        cost_estimate=pl.CostEstimate(flops=4 * 10**9, bytes_accessed=2 * 10**6, transcendentals=0),
        compiler_params=pltpu.CompilerParams(vmem_limit_bytes=24 * 2**20),
        name="left_prep",
    )(term_index, left_terms.transpose(1, 2, 3, 0), left_gates, as_rows(left_slabs, width), as_rows(left_other, width))

    pieces = {0: right}
    bit = count // 2
    while bit:
        for k in sorted(pieces):
            pieces[k | bit] = hop(pieces[k], bit)
        bit //= 2

    pairs = [jnp.concatenate([left[k + 1] for k in range(0, count, 2)], 0)]
    if count > 1:
        pairs = [hop(pairs[0], 1)]
    blocks = {}
    for k in range(0, count, 2):
        both = jnp.concatenate([left[k], pairs[0][k // 2 * part : (k // 2 + 1) * part]], 0)
        if k:
            both = hop(both, k)
        blocks[k], blocks[k + 1] = both[:part], both[part:]
    blocks = [blocks[k] for k in range(count)]
    rows = part * width
    own = pl.pallas_call(
        lambda *refs: arrange_kernel(count, *refs),
        in_specs=[VMEM] * count,
        out_specs=VMEM,
        out_shape=jax.ShapeDtypeStruct((2, rows, count * slots), BF16),
        cost_estimate=pl.CostEstimate(flops=2 * 10**9, bytes_accessed=10**6, transcendentals=0),
        compiler_params=pltpu.CompilerParams(vmem_limit_bytes=16 * 2**20),
        name="left_arrange",
    )(*blocks)
    other = swap(own)

    step = 4
    return pl.pallas_call(
        lambda *refs: contract_kernel(count, step, *refs),
        in_specs=[ANY] * (2 + count),
        out_specs=ANY,
        out_shape=jax.ShapeDtypeStruct((2, 2 * rows, groups * width), BF16),
        scratch_shapes=[
            pltpu.VMEM((2, 2 * rows, count * slots), BF16),
            pltpu.VMEM((groups, count * slots, width), BF16),
            pltpu.VMEM((4, 2, 2 * rows, step * width), BF16),
            pltpu.SemaphoreType.DMA((2 + count,)),
            pltpu.SemaphoreType.DMA((4,)),
        ],
        cost_estimate=pl.CostEstimate(flops=9 * 10**9, bytes_accessed=36 * 10**6, transcendentals=0),
        compiler_params=pltpu.CompilerParams(vmem_limit_bytes=40 * 2**20),
        name="contract",
    )(own, other, *[pieces[k] for k in range(count)])


def solution(mesh):
    return jax.shard_map(
        shards,
        mesh=mesh,
        in_specs=(
            P(("grp", "path"), None, "amp"),
            P(("grp", "path"), None, "amp"),
            P(("grp", "path")),
            P(),
            P(),
            P(),
            P(),
        ),
        out_specs=P(None, ("grp", "path"), "amp"),
        check_vma=False,
    )
```

```python
import functools

import jax
import jax.numpy as jnp
from jax import lax
from jax.experimental import pallas as pl
from jax.experimental.pallas import tpu as pltpu
from jax.sharding import PartitionSpec as P


F32 = jnp.float32
BF16 = jnp.bfloat16


def iota(shape, dim):
    return lax.broadcasted_iota(jnp.int32, shape, dim)


def one_hot(test):
    return jnp.where(test, 1.0, 0.0).astype(BF16)


def dot(a, b):
    return jnp.dot(a, b, preferred_element_type=F32)


def swap_pairs(x, axis):
    size = x.shape[axis]
    even = iota(x.shape, axis) % 2 == 0
    return jnp.where(even, pltpu.roll(x, size - 1, axis), pltpu.roll(x, 1, axis))


def swap_rows(x):
    rows, width = x.shape
    return swap_pairs(x.reshape(rows // 8, 8, width), 1).reshape(rows, width)


def row_sign(shape):
    return jnp.where(iota(shape, 0) % 2 == 0, -1.0, 1.0).astype(F32)


def stacked_gate(gates_ref, select, place):
    gate_width = gates_ref.shape[-1]
    columns = iota((gate_width, 2 * gate_width), 1)
    real_at = one_hot(columns == place)
    imag_at = one_hot(columns == place + 1)
    real = dot(select, gates_ref[1, 0]).astype(BF16)
    imag = dot(select, gates_ref[1, 1]).astype(BF16)
    top = dot(real, real_at) - dot(imag, imag_at)
    bottom = dot(imag, real_at) + dot(real, imag_at)
    return jnp.concatenate([top, bottom], 0).astype(BF16)


def cut_and_low(rows, path, table, index_ref, terms_ref, gates_ref):
    width = rows.shape[1]
    term = index_ref[path]
    parity = iota((1, width), 1) % 2 == 0

    def pattern(part, first, second):
        at = table + 4 * part
        return jnp.where(parity, terms_ref[at + first, term], terms_ref[at + 2 + second, term])

    sign = row_sign(rows.shape)
    value = rows.astype(F32)
    turned = swap_rows(value) * sign
    cut = (
        value * pattern(0, 0, 1)
        + turned * pattern(1, 0, 1)
        + swap_pairs(value, 1) * pattern(0, 1, 0)
        + swap_pairs(turned, 1) * pattern(1, 1, 0)
    ).astype(BF16)
    gate = gates_ref[0].reshape(2 * width, width)
    low = lax.dot_general(cut, gate, (((1,), (1,)), ((), ())), preferred_element_type=F32)
    return (low[:, :width] + swap_rows(low[:, width:]) * sign).astype(BF16)


def left_kernel(count, index_ref, terms_ref, gates_ref, slabs_ref, other_ref, *rest):
    out_refs, stage = rest[:count], rest[count]
    paths, size, width = other_ref.shape
    own_ref = slabs_ref.at[:, :size]
    mine, core = lax.axis_index("path"), lax.axis_index("amp")
    half = width // 2
    part = half // count
    which = iota((half, width), 0)
    target = ((which // part) ^ mine) * (2 * part) + core * part + which % part
    select = one_hot(iota((half, width), 1) == target)
    source = iota((width, 2 * width), 0)
    place = ((source // half) ^ core) * width + (source % half) * 2
    matrix = stacked_gate(gates_ref, select, place)
    slots = 2 * paths

    for pair in range(0, paths, 2):
        columns = []
        for path in (pair, pair + 1):
            parts = [
                cut_and_low(ref[path], path, 8, index_ref, terms_ref, gates_ref)
                for ref in (own_ref, other_ref)
            ]
            columns.append(jnp.concatenate(parts, 0))
        turned = dot(matrix, jnp.concatenate(columns, 1))
        for at, path in enumerate((pair, pair + 1)):
            for ri in range(2):
                stage[pl.ds(ri * paths + path, half, stride=slots), :] = turned[
                    ri * half : (ri + 1) * half, at * width : (at + 1) * width
                ]
    for k in range(count):
        rows = stage[k * part * slots : (k + 1) * part * slots, :]
        out_refs[k][...] = rows.astype(BF16).reshape(part, slots, width)


def right_kernel(index_ref, terms_ref, gates_ref, slabs_ref, other_ref, out_ref, stage):
    paths, size, width = other_ref.shape
    own_ref = slabs_ref.at[:, slabs_ref.shape[1] - size :]
    core = lax.axis_index("amp")
    half, quarter = width // 2, width // 4
    which = iota((half, width), 0)
    target = 2 * (core * quarter + which % quarter) + which // quarter
    select = one_hot(iota((half, width), 1) == target)
    source = iota((width, 2 * width), 0)
    group = source // 2
    place = (source % 2) * width + ((group // quarter) ^ core) * half + (group % quarter) * 2
    matrix = stacked_gate(gates_ref, select, place)
    slots = 2 * paths
    front = iota((1, width), 1) < half

    for four in range(0, paths, 4):
        columns = []
        for pair in (four, four + 2):
            first, second = [
                jnp.concatenate(
                    [
                        cut_and_low(ref[path], path, 0, index_ref, terms_ref, gates_ref)
                        for ref in (own_ref, other_ref)
                    ],
                    0,
                ).astype(F32)
                for path in (pair, pair + 1)
            ]
            upper = jnp.where(front, first, pltpu.roll(second, half, 1))
            lower = jnp.where(front, pltpu.roll(first, half, 1), second)
            columns.append(jnp.concatenate([upper, lower], 0).astype(BF16))
        turned = dot(matrix, jnp.concatenate(columns, 1))
        for at, pair in enumerate((four, four + 2)):
            for ri in range(2):
                block = turned[ri * half : (ri + 1) * half, at * width : (at + 1) * width]
                upper, lower = block[:quarter], block[quarter:]
                stage[pl.ds(ri * paths + pair, quarter, stride=slots), :] = jnp.where(
                    front, upper, pltpu.roll(lower, half, 1)
                )
                stage[pl.ds(ri * paths + pair + 1, quarter, stride=slots), :] = jnp.where(
                    front, pltpu.roll(upper, half, 1), lower
                )
    out_ref[...] = stage[...].astype(BF16).reshape(out_ref.shape)


def arrange_kernel(count, *refs):
    blocks, out_ref = refs[:count], refs[count]
    part, slots, width = blocks[0].shape
    paths = slots // 2
    for j in range(part):
        plain, crossed = [], []
        for ref in blocks:
            block = ref[j].astype(F32)
            real, imag = block[:paths], block[paths:]
            plain += [real, -imag]
            crossed += [imag, real]
        for at, rows in enumerate((plain, crossed)):
            out_ref[at, j * width : (j + 1) * width, :] = jnp.concatenate(rows, 0).T.astype(BF16)


def contract_kernel(count, step, own_ref, other_ref, *refs):
    pieces, out_ref = refs[:count], refs[count]
    left, right, staged, in_sems, out_sems = refs[count + 1 :]
    core = lax.axis_index("amp")
    rows = own_ref.shape[1]
    groups, slots, width = pieces[0].shape
    span = step * width
    copies = [
        pltpu.make_async_copy(
            ref, left.at[:, pl.ds(pl.multiple_of(where * rows, rows), rows), :], in_sems.at[at]
        )
        for at, (ref, where) in enumerate(((own_ref, core), (other_ref, 1 - core)))
    ] + [
        pltpu.make_async_copy(piece, right.at[:, pl.ds(k * slots, slots), :], in_sems.at[2 + k])
        for k, piece in enumerate(pieces)
    ]
    for copy in copies:
        copy.start()
    for copy in copies:
        copy.wait()
    buffers = staged.shape[0]

    def write(i, slot):
        place = pl.ds(pl.multiple_of(i * span, span), span)
        return pltpu.make_async_copy(staged.at[slot], out_ref.at[:, :, place], out_sems.at[slot])

    tile = min(256, 2 * rows)

    @pl.loop(0, groups // step)
    def _(i):
        slot = lax.rem(i, buffers)

        @pl.when(i >= buffers)
        def _():
            write(i - buffers, slot).wait()

        block = jnp.concatenate([right[i * step + g] for g in range(step)], 1)
        for part in range(2):
            for start in range(0, 2 * rows, tile):
                staged[slot, part, start : start + tile, :] = dot(
                    left[part, start : start + tile, :], block
                ).astype(BF16)
        write(i, slot).start()

    for i in range(groups // step - buffers, groups // step):
        write(i, i % buffers).wait()


SMEM = pl.BlockSpec(memory_space=pltpu.SMEM)
VMEM = pl.BlockSpec(memory_space=pltpu.VMEM)
ANY = pl.BlockSpec(memory_space=pl.ANY)
HBM = pl.BlockSpec(memory_space=pltpu.HBM)


def as_rows(slab, width):
    paths, _, length = slab.shape
    groups = length // width
    return slab.reshape(paths, 2, groups, width).transpose(0, 2, 1, 3).reshape(paths, 2 * groups, width)


def shards(left_slabs, right_slabs, term_index, left_terms, right_terms, left_gates, right_gates):
    width = left_gates.shape[-1]
    count = lax.axis_size("path")
    paths = left_slabs.shape[0]
    slots = 2 * paths

    def swap(x):
        return lax.ppermute(x, "amp", [(0, 1), (1, 0)])

    def hop(x, k):
        return lax.ppermute(x, "path", [(i, i ^ k) for i in range(count)])

    right_other = swap(right_slabs)
    left_other = swap(left_slabs)

    groups = right_slabs.shape[2] // width
    part = width // 2 // count
    slabs = as_rows(jnp.concatenate([left_slabs, right_slabs], 2), width)
    terms = jnp.concatenate(
        [terms.transpose(1, 2, 3, 0).reshape(8, -1) for terms in (right_terms, left_terms)], 0
    )
    right = pl.pallas_call(
        right_kernel,
        in_specs=[SMEM, SMEM, VMEM, VMEM, VMEM],
        out_specs=VMEM,
        out_shape=jax.ShapeDtypeStruct((groups, slots, width), BF16),
        scratch_shapes=[pltpu.VMEM((groups * slots, width), F32)],
        cost_estimate=pl.CostEstimate(flops=2 * 10**9, bytes_accessed=10**6, transcendentals=0),
        compiler_params=pltpu.CompilerParams(vmem_limit_bytes=24 * 2**20),
        name="right_prep",
    )(term_index, terms, right_gates, slabs, as_rows(right_other, width))
    left = pl.pallas_call(
        functools.partial(left_kernel, count),
        in_specs=[SMEM, SMEM, VMEM, VMEM, VMEM],
        out_specs=[VMEM] * count,
        out_shape=[jax.ShapeDtypeStruct((part, slots, width), BF16)] * count,
        scratch_shapes=[pltpu.VMEM((width // 2 * slots, width), F32)],
        cost_estimate=pl.CostEstimate(flops=4 * 10**9, bytes_accessed=2 * 10**6, transcendentals=0),
        compiler_params=pltpu.CompilerParams(vmem_limit_bytes=24 * 2**20),
        name="left_prep",
    )(term_index, terms, left_gates, slabs, as_rows(left_other, width))

    pieces = {0: right}
    bit = count // 2
    while bit:
        for k in sorted(pieces):
            pieces[k | bit] = hop(pieces[k], bit)
        bit //= 2

    pairs = [jnp.concatenate([left[k + 1] for k in range(0, count, 2)], 0)]
    if count > 1:
        pairs = [hop(pairs[0], 1)]
    blocks = {}
    for k in range(0, count, 2):
        both = jnp.concatenate([left[k], pairs[0][k // 2 * part : (k // 2 + 1) * part]], 0)
        if k:
            both = hop(both, k)
        blocks[k], blocks[k + 1] = both[:part], both[part:]
    rows = part * width
    own = pl.pallas_call(
        functools.partial(arrange_kernel, count),
        in_specs=[VMEM] * count,
        out_specs=VMEM,
        out_shape=jax.ShapeDtypeStruct((2, rows, count * slots), BF16),
        cost_estimate=pl.CostEstimate(flops=10**9, bytes_accessed=10**6, transcendentals=0),
        compiler_params=pltpu.CompilerParams(vmem_limit_bytes=16 * 2**20),
        name="left_arrange",
    )(*[blocks[k] for k in range(count)])
    other = swap(own)
    step = 4
    return pl.pallas_call(
        lambda *refs: contract_kernel(count, step, *refs),
        in_specs=[ANY] * (2 + count),
        out_specs=ANY,
        out_shape=jax.ShapeDtypeStruct((2, 2 * rows, groups * width), BF16),
        scratch_shapes=[
            pltpu.VMEM((2, 2 * rows, count * slots), BF16),
            pltpu.VMEM((groups, count * slots, width), BF16),
            pltpu.VMEM((4, 2, 2 * rows, step * width), BF16),
            pltpu.SemaphoreType.DMA((2 + count,)),
            pltpu.SemaphoreType.DMA((4,)),
        ],
        cost_estimate=pl.CostEstimate(flops=9 * 10**9, bytes_accessed=36 * 10**6, transcendentals=0),
        compiler_params=pltpu.CompilerParams(vmem_limit_bytes=40 * 2**20),
        name="contract",
    )(own, other, *[pieces[k] for k in range(count)])


def solution(mesh):
    return jax.shard_map(
        shards,
        mesh=mesh,
        in_specs=(
            P(("grp", "path"), None, "amp"),
            P(("grp", "path"), None, "amp"),
            P(("grp", "path")),
            P(),
            P(),
            P(),
            P(),
        ),
        out_specs=P(None, ("grp", "path"), "amp"),
        check_vma=False,
    )
```

```python
import functools

import jax
import jax.numpy as jnp
from jax import lax
from jax.experimental import pallas as pl
from jax.experimental.pallas import tpu as pltpu
from jax.sharding import PartitionSpec as P


F32 = jnp.float32
BF16 = jnp.bfloat16


def iota(shape, dim):
    return lax.broadcasted_iota(jnp.int32, shape, dim)


def one_hot(test):
    return jnp.where(test, 1.0, 0.0).astype(BF16)


def dot(a, b):
    return jnp.dot(a, b, preferred_element_type=F32)


def swap_pairs(x, axis):
    size = x.shape[axis]
    even = iota(x.shape, axis) % 2 == 0
    return jnp.where(even, pltpu.roll(x, size - 1, axis), pltpu.roll(x, 1, axis))


def swap_rows(x):
    rows, width = x.shape
    return swap_pairs(x.reshape(rows // 8, 8, width), 1).reshape(rows, width)


def row_sign(shape):
    return jnp.where(iota(shape, 0) % 2 == 0, -1.0, 1.0).astype(F32)


def stacked_gate(gates_ref, select, place):
    gate_width = gates_ref.shape[-1]
    columns = iota((gate_width, 2 * gate_width), 1)
    real_at = one_hot(columns == place)
    imag_at = one_hot(columns == place + 1)
    real = dot(select, gates_ref[1, 0]).astype(BF16)
    imag = dot(select, gates_ref[1, 1]).astype(BF16)
    top = dot(real, real_at) - dot(imag, imag_at)
    bottom = dot(imag, real_at) + dot(real, imag_at)
    return jnp.concatenate([top, bottom], 0).astype(BF16)


def cut_and_low(rows, path, table, index_ref, terms_ref, gates_ref):
    width = rows.shape[1]
    term = index_ref[path]
    parity = iota((1, width), 1) % 2 == 0

    def pattern(part, first, second):
        at = table + 4 * part
        return jnp.where(parity, terms_ref[at + first, term], terms_ref[at + 2 + second, term])

    sign = row_sign(rows.shape)
    value = rows.astype(F32)
    turned = swap_rows(value) * sign
    cut = (
        value * pattern(0, 0, 1)
        + turned * pattern(1, 0, 1)
        + swap_pairs(value, 1) * pattern(0, 1, 0)
        + swap_pairs(turned, 1) * pattern(1, 1, 0)
    ).astype(BF16)
    gate = gates_ref[0].reshape(2 * width, width)
    low = lax.dot_general(cut, gate, (((1,), (1,)), ((), ())), preferred_element_type=F32)
    return (low[:, :width] + swap_rows(low[:, width:]) * sign).astype(BF16)


def left_kernel(count, index_ref, terms_ref, gates_ref, slabs_ref, other_ref, *rest):
    out_refs, stage = rest[:count], rest[count]
    paths, size, width = other_ref.shape
    own_ref = slabs_ref.at[:, :size]
    mine, core = lax.axis_index("path"), lax.axis_index("amp")
    half = width // 2
    part = half // count
    which = iota((half, width), 0)
    target = ((which // part) ^ mine) * (2 * part) + core * part + which % part
    select = one_hot(iota((half, width), 1) == target)
    source = iota((width, 2 * width), 0)
    place = ((source // half) ^ core) * width + (source % half) * 2
    matrix = stacked_gate(gates_ref, select, place)
    slots = 2 * paths

    for pair in range(0, paths, 2):
        columns = []
        for path in (pair, pair + 1):
            parts = [
                cut_and_low(ref[path], path, 8, index_ref, terms_ref, gates_ref)
                for ref in (own_ref, other_ref)
            ]
            columns.append(jnp.concatenate(parts, 0))
        turned = dot(matrix, jnp.concatenate(columns, 1))
        for at, path in enumerate((pair, pair + 1)):
            for ri in range(2):
                stage[pl.ds(ri * paths + path, half, stride=slots), :] = turned[
                    ri * half : (ri + 1) * half, at * width : (at + 1) * width
                ]
    for k in range(count):
        rows = stage[k * part * slots : (k + 1) * part * slots, :]
        out_refs[k][...] = rows.astype(BF16).reshape(part, slots, width)


def right_kernel(index_ref, terms_ref, gates_ref, slabs_ref, other_ref, out_ref, stage):
    paths, size, width = other_ref.shape
    own_ref = slabs_ref.at[:, slabs_ref.shape[1] - size :]
    core = lax.axis_index("amp")
    half, quarter = width // 2, width // 4
    which = iota((half, width), 0)
    target = 2 * (core * quarter + which % quarter) + which // quarter
    select = one_hot(iota((half, width), 1) == target)
    source = iota((width, 2 * width), 0)
    group = source // 2
    place = (source % 2) * width + ((group // quarter) ^ core) * half + (group % quarter) * 2
    matrix = stacked_gate(gates_ref, select, place)
    slots = 2 * paths
    front = iota((1, width), 1) < half

    for four in range(0, paths, 4):
        columns = []
        for pair in (four, four + 2):
            first, second = [
                jnp.concatenate(
                    [
                        cut_and_low(ref[path], path, 0, index_ref, terms_ref, gates_ref)
                        for ref in (own_ref, other_ref)
                    ],
                    0,
                ).astype(F32)
                for path in (pair, pair + 1)
            ]
            upper = jnp.where(front, first, pltpu.roll(second, half, 1))
            lower = jnp.where(front, pltpu.roll(first, half, 1), second)
            columns.append(jnp.concatenate([upper, lower], 0).astype(BF16))
        turned = dot(matrix, jnp.concatenate(columns, 1))
        for at, pair in enumerate((four, four + 2)):
            for ri in range(2):
                block = turned[ri * half : (ri + 1) * half, at * width : (at + 1) * width]
                upper, lower = block[:quarter], block[quarter:]
                stage[pl.ds(ri * paths + pair, quarter, stride=slots), :] = jnp.where(
                    front, upper, pltpu.roll(lower, half, 1)
                )
                stage[pl.ds(ri * paths + pair + 1, quarter, stride=slots), :] = jnp.where(
                    front, pltpu.roll(upper, half, 1), lower
                )
    out_ref[...] = stage[...].astype(BF16).reshape(out_ref.shape)


def arrange_kernel(count, *refs):
    blocks, out_ref = refs[:count], refs[count]
    part, slots, width = blocks[0].shape
    paths = slots // 2
    for j in range(part):
        plain, crossed = [], []
        for ref in blocks:
            block = ref[j].astype(F32)
            real, imag = block[:paths], block[paths:]
            plain += [real, -imag]
            crossed += [imag, real]
        for at, rows in enumerate((plain, crossed)):
            out_ref[at, j * width : (j + 1) * width, :] = jnp.concatenate(rows, 0).T.astype(BF16)


def contract_kernel(count, step, own_ref, other_ref, *refs):
    pieces = refs[:count]
    out_ref, staged, sems = refs[count:]
    core = lax.axis_index("amp")
    rows = own_ref.shape[1]
    groups, _, width = pieces[0].shape
    span = step * width
    tile = min(256, rows)
    buffers = staged.shape[0]

    def write(i, slot, half, part):
        place = pl.ds(pl.multiple_of(i * span, span), span)
        where = pl.ds(pl.multiple_of((core ^ half) * rows, rows), rows)
        return pltpu.make_async_copy(
            staged.at[slot, half, part], out_ref.at[part, where, place], sems.at[slot, half, part]
        )

    quarters = [(half, part) for half in range(2) for part in range(2)]

    @pl.loop(0, groups // step)
    def _(i):
        slot = lax.rem(i, buffers)

        @pl.when(i >= buffers)
        def _():
            for quarter in quarters:
                write(i - buffers, slot, *quarter).wait()

        block = jnp.concatenate(
            [jnp.concatenate([piece[i * step + g] for piece in pieces], 0) for g in range(step)], 1
        )
        for half, part in quarters:
            ref = (own_ref, other_ref)[half]
            for start in range(0, rows, tile):
                staged[slot, half, part, start : start + tile, :] = dot(
                    ref[part, start : start + tile, :], block
                ).astype(BF16)
            write(i, slot, half, part).start()

    for i in range(groups // step - buffers, groups // step):
        for quarter in quarters:
            write(i, i % buffers, *quarter).wait()


SMEM = pl.BlockSpec(memory_space=pltpu.SMEM)
VMEM = pl.BlockSpec(memory_space=pltpu.VMEM)
ANY = pl.BlockSpec(memory_space=pl.ANY)
HBM = pl.BlockSpec(memory_space=pltpu.HBM)


def as_rows(slab, width):
    paths, _, length = slab.shape
    groups = length // width
    return slab.reshape(paths, 2, groups, width).transpose(0, 2, 1, 3).reshape(paths, 2 * groups, width)


def shards(left_slabs, right_slabs, term_index, left_terms, right_terms, left_gates, right_gates):
    width = left_gates.shape[-1]
    count = lax.axis_size("path")
    paths = left_slabs.shape[0]
    slots = 2 * paths

    def swap(x):
        return lax.ppermute(x, "amp", [(0, 1), (1, 0)])

    def hop(x, k):
        return lax.ppermute(x, "path", [(i, i ^ k) for i in range(count)])

    right_other = swap(right_slabs)
    left_other = swap(left_slabs)

    groups = right_slabs.shape[2] // width
    part = width // 2 // count
    slabs = as_rows(jnp.concatenate([left_slabs, right_slabs], 2), width)
    terms = jnp.concatenate(
        [terms.transpose(1, 2, 3, 0).reshape(8, -1) for terms in (right_terms, left_terms)], 0
    )
    right = pl.pallas_call(
        right_kernel,
        in_specs=[SMEM, SMEM, VMEM, VMEM, VMEM],
        out_specs=VMEM,
        out_shape=jax.ShapeDtypeStruct((groups, slots, width), BF16),
        scratch_shapes=[pltpu.VMEM((groups * slots, width), F32)],
        cost_estimate=pl.CostEstimate(flops=2 * 10**9, bytes_accessed=10**6, transcendentals=0),
        compiler_params=pltpu.CompilerParams(vmem_limit_bytes=24 * 2**20),
        name="right_prep",
    )(term_index, terms, right_gates, slabs, as_rows(right_other, width))
    left = pl.pallas_call(
        functools.partial(left_kernel, count),
        in_specs=[SMEM, SMEM, VMEM, VMEM, VMEM],
        out_specs=[VMEM] * count,
        out_shape=[jax.ShapeDtypeStruct((part, slots, width), BF16)] * count,
        scratch_shapes=[pltpu.VMEM((width // 2 * slots, width), F32)],
        cost_estimate=pl.CostEstimate(flops=4 * 10**9, bytes_accessed=2 * 10**6, transcendentals=0),
        compiler_params=pltpu.CompilerParams(vmem_limit_bytes=24 * 2**20),
        name="left_prep",
    )(term_index, terms, left_gates, slabs, as_rows(left_other, width))

    pieces = {0: right}
    bit = count // 2
    while bit:
        for k in sorted(pieces):
            pieces[k | bit] = hop(pieces[k], bit)
        bit //= 2

    pairs = [jnp.concatenate([left[k + 1] for k in range(0, count, 2)], 0)]
    if count > 1:
        pairs = [hop(pairs[0], 1)]
    blocks = {}
    for k in range(0, count, 2):
        both = jnp.concatenate([left[k], pairs[0][k // 2 * part : (k // 2 + 1) * part]], 0)
        if k:
            both = hop(both, k)
        blocks[k], blocks[k + 1] = both[:part], both[part:]
    rows = part * width
    own = pl.pallas_call(
        functools.partial(arrange_kernel, count),
        in_specs=[VMEM] * count,
        out_specs=VMEM,
        out_shape=jax.ShapeDtypeStruct((2, rows, count * slots), BF16),
        cost_estimate=pl.CostEstimate(flops=10**9, bytes_accessed=10**6, transcendentals=0),
        compiler_params=pltpu.CompilerParams(vmem_limit_bytes=16 * 2**20),
        name="left_arrange",
    )(*[blocks[k] for k in range(count)])
    other = swap(own)
    step = 4
    return pl.pallas_call(
        lambda *refs: contract_kernel(count, step, *refs),
        in_specs=[VMEM] * (2 + count),
        out_specs=ANY,
        out_shape=jax.ShapeDtypeStruct((2, 2 * rows, groups * width), BF16),
        scratch_shapes=[
            pltpu.VMEM((4, 2, 2, rows, step * width), BF16),
            pltpu.SemaphoreType.DMA((4, 2, 2)),
        ],
        cost_estimate=pl.CostEstimate(flops=9 * 10**9, bytes_accessed=36 * 10**6, transcendentals=0),
        compiler_params=pltpu.CompilerParams(vmem_limit_bytes=40 * 2**20),
        name="contract",
    )(own, other, *[pieces[k] for k in range(count)])


def solution(mesh):
    return jax.shard_map(
        shards,
        mesh=mesh,
        in_specs=(
            P(("grp", "path"), None, "amp"),
            P(("grp", "path"), None, "amp"),
            P(("grp", "path")),
            P(),
            P(),
            P(),
            P(),
        ),
        out_specs=P(None, ("grp", "path"), "amp"),
        check_vma=False,
    )
```
